32 devices in a mesh: tile: 8 (over z, y), lev: 4 (over x, core).
Axes of the slice: x: 2, y: 2, z: 4, core: 2. Of those that a mesh axis runs over, the one named last changes fastest.
Arguments:
- ensemble: bfloat16 [80, 32, 4096], P(None, 'lev', 'tile')
- pair_first: int32 [32768], P('tile'), may hold values from 0 to 511
- pair_second: int32 [32768], P('tile'), may hold values from 0 to 1023
- pair_bin: int32 [32768], P('tile'), may hold values from 0 to 63, as said below
Outputs:
- level_variance: float32 [32], P('lev')
- bin_corr: float32 [32, 64], P('lev', 'tile')
- bin_avg: float32 [64], P('tile')
The draws below stay inside these ranges and needn't reach their ends.
Inputs may be any that keep to these rules, and one draw needn't show every extreme that they name: `pair_bin`: some bins receive no pair; which ones changes with the draw.
All inputs are finite; a program needn't handle non-finite values.
Results may differ from the reference program's by a relative error of at most 0.0017.
Values may be sent and summed in bfloat16 or wider, within the bound.
A program may use at most 64 MiB of HBM per device.

```python
import jax
import jax.numpy as jnp
from jax import lax

MEMBERS = 80
LEVELS = 32
COL_DEV = 512
PAIRS_DEV = 4096
COLS = 4096
NPAIRS = 32768
NBINS = 64


def draw_ensemble(key, part):
    keys = jax.random.split(jax.random.fold_in(key, 7), 5)
    level_scale = jnp.exp(jax.random.uniform(keys[0], (1, LEVELS, 1), jnp.float32, -1.2, 1.2))
    factor = jax.random.normal(keys[1], (MEMBERS, LEVELS, 2), jnp.float32)
    loading = jax.random.uniform(keys[2], (2, LEVELS, COLS), jnp.float32, -1.2, 1.2)
    offset = 2.0 * jax.random.normal(keys[4], (1, LEVELS, COLS), jnp.float32)
    noise = jax.random.normal(keys[3], (MEMBERS, LEVELS, COLS), jnp.float32)
    colscale = jnp.ones((1, 1, COLS), jnp.float32)
    shared = factor[:, :, 0:1] * loading[0][None] + factor[:, :, 1:2] * loading[1][None]
    return (level_scale * colscale * (shared + noise) + offset).astype(jnp.bfloat16)


def draw_pair_bin(key, part):
    keys = jax.random.split(jax.random.fold_in(key, 11), 3)
    skipped = NBINS // 8
    inner = (1 + jax.random.permutation(keys[0], NBINS - 2)).astype(jnp.int32)
    kept = inner[skipped:]
    half = kept.shape[0] // 2
    ends = jnp.array([0, NBINS - 1], dtype=jnp.int32)
    table = jnp.concatenate([kept[:half], ends, kept[half:]])
    allowed = table.shape[0]
    first = jax.random.randint(keys[1], (NPAIRS,), 0, allowed, dtype=jnp.int32)
    second = jax.random.randint(keys[2], (NPAIRS,), 0, allowed, dtype=jnp.int32)
    rank = jnp.minimum(first, second)
    return jnp.take(table, rank).astype(jnp.int32)


def place_ends(values, stream_key, smallest, largest):
    spot = [jax.random.randint(jax.random.fold_in(stream_key, axis), (), 0, length) for axis, length in enumerate(values.shape)]
    longest = values.shape.index(max(values.shape))
    beside = spot[:longest] + [(spot[longest] + 1) % values.shape[longest]] + spot[longest + 1:]
    return values.at[tuple(spot)].set(smallest).at[tuple(beside)].set(largest)


def setup_inputs(seed: int = 0) -> dict:
    streams_of = jax.random.split(jax.random.key(seed), 5)
    ensemble = draw_ensemble(jax.random.fold_in(streams_of[4], 71), 0)
    pair_first = place_ends(jax.random.randint(streams_of[1], (NPAIRS,), 0, COL_DEV), jax.random.fold_in(streams_of[1], 1), 0, COL_DEV - 1).astype(jnp.int32)
    pair_second = place_ends(jax.random.randint(streams_of[2], (NPAIRS,), 0, 2 * COL_DEV), jax.random.fold_in(streams_of[2], 1), 0, (2 * COL_DEV) - 1).astype(jnp.int32)
    pair_bin = draw_pair_bin(jax.random.fold_in(streams_of[4], 71), 0)
    return {"ensemble": ensemble, "pair_first": pair_first, "pair_second": pair_second, "pair_bin": pair_bin}


def perturb(block):
    values = block.astype(jnp.float32)
    return (values - lax.optimization_barrier(jnp.mean(values, axis=0, keepdims=True))).astype(jnp.bfloat16)

def reference(ensemble, pair_first, pair_second, pair_bin):
    ntile = COLS // COL_DEV

    def tile_terms(tile):
        own = lax.dynamic_slice_in_dim(ensemble, (tile * COL_DEV).astype(jnp.int32), COL_DEV, 2)
        nxt = lax.dynamic_slice_in_dim(ensemble, ((tile + 1) % ntile * COL_DEV).astype(jnp.int32), COL_DEV, 2)
        pert_own = perturb(own).astype(jnp.float32)
        pert_ext = jnp.concatenate([pert_own, perturb(nxt).astype(jnp.float32)], axis=2)
        spread = jnp.sqrt(lax.optimization_barrier(jnp.sum(pert_ext * pert_ext, axis=0)) / (MEMBERS - 1) + 1e-06)
        squares = lax.optimization_barrier(jnp.sum(pert_own * pert_own, axis=(0, 2)))
        start = (tile * PAIRS_DEV).astype(jnp.int32)
        first = lax.dynamic_slice_in_dim(pair_first, start, PAIRS_DEV, 0)
        second = lax.dynamic_slice_in_dim(pair_second, start, PAIRS_DEV, 0)
        bins = lax.dynamic_slice_in_dim(pair_bin, start, PAIRS_DEV, 0)
        left = jnp.take(pert_ext, first, axis=2)
        right = jnp.take(pert_ext, second, axis=2)
        cov = lax.optimization_barrier(jnp.sum(left * right, axis=0)) / (MEMBERS - 1)
        corr = cov / (jnp.take(spread, first, axis=1) * jnp.take(spread, second, axis=1))
        onehot = (bins[:, None] == jnp.arange(NBINS, dtype=jnp.int32)[None, :]).astype(jnp.float32)
        sums = jnp.dot(corr, onehot, precision=lax.Precision.HIGHEST)
        return (sums, lax.optimization_barrier(jnp.sum(onehot, axis=0)), squares)
    sums, counts, squares = lax.map(tile_terms, jnp.arange(ntile, dtype=jnp.int32))
    bin_sum = lax.optimization_barrier(jnp.sum(sums, axis=0))
    bin_count = lax.optimization_barrier(jnp.sum(counts, axis=0))
    level_variance = lax.optimization_barrier(jnp.sum(squares, axis=0)) / ((MEMBERS - 1) * COLS)
    bin_corr = bin_sum / jnp.maximum(bin_count, 1.0)[None, :]
    bin_avg = lax.optimization_barrier(jnp.sum(level_variance[:, None] * bin_corr, axis=0)) / jnp.sum(level_variance)
    return (level_variance, bin_corr, bin_avg)
```

```python
import functools

import jax
import jax.numpy as jnp
from jax import lax
from jax.experimental import pallas as pl
from jax.experimental.pallas import tpu as pltpu
from jax.sharding import PartitionSpec as P

BIN_DEV = 8
LANES = 128
PAIR_CHUNK = 512
HALO_CHUNKS = 2


def pieces3(x):
    a = x.astype(jnp.bfloat16).astype(jnp.float32)
    r = x - a
    b = r.astype(jnp.bfloat16).astype(jnp.float32)
    return a, b, r - b


def onehot(rows, base, count):
    ids = lax.broadcasted_iota(jnp.int32, (count, LANES), 0) + base
    parts = [jnp.where(ids == r, 1.0, 0.0) for r in rows]
    return jnp.concatenate(parts, axis=1).astype(jnp.bfloat16)


def perturb(raw, out, squares, width):
    members, lev = raw.shape[0], raw.shape[1]
    rows = members * lev
    for c in range(0, width, LANES):
        cs = pl.ds(c, LANES)
        x = raw[:, :, cs].astype(jnp.float32)
        mean = jnp.sum(x, axis=0) / members
        pert = (x - mean[None]).astype(jnp.bfloat16).astype(jnp.float32)
        sq = jnp.sum(pert * pert, axis=0)
        out[pl.ds(0, rows), cs] = pert.reshape(rows, LANES).astype(jnp.bfloat16)
        inv = 1.0 / jnp.sqrt(sq / (members - 1) + 1e-06)
        hi = inv.astype(jnp.bfloat16).astype(jnp.float32)
        out[pl.ds(rows, 2 * lev), cs] = jnp.concatenate([hi, inv - hi], axis=0).astype(jnp.bfloat16)
        if squares is not None:
            squares[:, cs] = sq


def kernel(
    ntile, nlev, ens, first_in, second_in, bin_in, lv_out, corr_out, avg_out,
    raw, halo, first, second, bins, own, nxt, squares, left_buf, cov_buf, ia_buf, ib_buf,
    bacc, sbuf, rbuf, lsend, lrecv,
    load_sem, halo_send, halo_recv, t_send, t_recv, l_send, l_recv,
):
    members, lev, cols = ens.shape
    rows = members * lev
    half = cols // HALO_CHUNKS
    total_bins = BIN_DEV * ntile
    chunks = left_buf.shape[0]
    groups = PAIR_CHUNK // LANES
    me = lax.axis_index("tile")
    my_lev = lax.axis_index("lev")

    barrier = pltpu.get_barrier_semaphore()
    for d in range(1, ntile):
        pl.semaphore_signal(
            barrier, inc=1, device_id=(lax.rem(me + d, ntile), my_lev),
            device_id_type=pl.DeviceIdType.MESH,
        )
    for d in range(1, nlev):
        pl.semaphore_signal(
            barrier, inc=1, device_id=(me, lax.rem(my_lev + d, nlev)),
            device_id_type=pl.DeviceIdType.MESH,
        )
    loads = [
        pltpu.make_async_copy(s, d, load_sem.at[i])
        for i, (s, d) in enumerate(
            ((ens, raw), (first_in, first), (second_in, second), (bin_in, bins))
        )
    ]
    for c in loads:
        c.start()
    loads[0].wait()
    pl.semaphore_wait(barrier, ntile - 1 + nlev - 1)
    prev = lax.rem(me + ntile - 1, ntile)
    halos = [
        pltpu.make_async_remote_copy(
            src_ref=raw.at[:, :, pl.ds(h * half, half)],
            dst_ref=halo.at[h],
            send_sem=halo_send.at[h],
            recv_sem=halo_recv.at[h],
            device_id=(prev, my_lev),
            device_id_type=pl.DeviceIdType.MESH,
        )
        for h in range(HALO_CHUNKS)
    ]
    for c in halos:
        c.start()
    for c in loads[1:]:
        c.wait()

    perturb(raw, own, squares, cols)

    def index_rows(ref, j):
        return [ref[pl.ds(j * groups + i, 1), :] for i in range(groups)]

    def product(a, b):
        return jnp.sum((a * b).reshape(members, lev, PAIR_CHUNK), axis=0)

    def own_step(j, carry):
        x = own[...]
        left = jnp.dot(x, onehot(index_rows(first, j), 0, cols), preferred_element_type=jnp.float32)
        left_buf[j] = left[:rows]
        right = jnp.dot(x, onehot(index_rows(second, j), 0, cols), preferred_element_type=jnp.float32)
        cov_buf[j] = product(left_buf[j], right[:rows])
        ia_buf[j] = left[rows:rows + lev] + left[rows + lev:]
        ib_buf[j] = right[rows:rows + lev] + right[rows + lev:]
        return carry

    lax.fori_loop(0, chunks, own_step, 0)
    bacc[...] = jnp.zeros_like(bacc)

    for h in range(HALO_CHUNKS):
        halos[h].wait_recv()
        perturb(halo.at[h], nxt.at[h], None, half)

        def next_step(j, carry):
            oh = onehot(index_rows(second, j), cols + h * half, half)
            right = jnp.dot(nxt[h], oh, preferred_element_type=jnp.float32)
            cov = cov_buf[j] + product(left_buf[j], right[:rows])
            ib = ib_buf[j] + right[rows:rows + lev] + right[rows + lev:]
            if h < HALO_CHUNKS - 1:
                cov_buf[j] = cov
                ib_buf[j] = ib
            else:
                corr = cov * ia_buf[j] * ib / (members - 1)
                parts = jnp.concatenate(
                    [*pieces3(corr), jnp.ones_like(corr),
                     jnp.zeros((LANES - 4 * lev, PAIR_CHUNK), jnp.float32)], axis=0
                ).astype(jnp.bfloat16)
                oh = onehot(index_rows(bins, j), 0, total_bins)
                bacc[...] += lax.dot_general(
                    oh, parts, (((1,), (1,)), ((), ())), preferred_element_type=jnp.float32
                )
            return carry

        lax.fori_loop(0, chunks, next_step, 0)

    sq_parts = jnp.concatenate(
        [jnp.zeros((4 * lev, cols), jnp.float32), *pieces3(squares[...]),
         jnp.zeros((LANES - 7 * lev, cols), jnp.float32)], axis=0
    ).astype(jnp.bfloat16)
    sq_row = lax.dot_general(
        jnp.ones((16, cols), jnp.bfloat16), sq_parts, (((1,), (1,)), ((), ())),
        preferred_element_type=jnp.float32,
    )[:BIN_DEV]
    for t in range(ntile):
        sbuf[t] = bacc[pl.ds(t * BIN_DEV, BIN_DEV), :] + sq_row
    rbuf[me] = sbuf[me]

    def t_copy(d):
        peer = lax.rem(me + d, ntile)
        return pltpu.make_async_remote_copy(
            src_ref=sbuf.at[peer], dst_ref=rbuf.at[me],
            send_sem=t_send.at[d], recv_sem=t_recv.at[me],
            device_id=(peer, my_lev), device_id_type=pl.DeviceIdType.MESH,
        )

    for d in range(1, ntile):
        t_copy(d).start()
    for d in range(1, ntile):
        src = lax.rem(me + d, ntile)
        pltpu.make_async_copy(rbuf.at[src], rbuf.at[src], t_recv.at[src]).wait()
    tot = rbuf[0]
    for t in range(1, ntile):
        tot = tot + rbuf[t]
    lane = lax.broadcasted_iota(jnp.int32, (BIN_DEV, LANES), 1)
    s = tot + pltpu.roll(tot, LANES - lev, 1) + pltpu.roll(tot, LANES - 2 * lev, 1)
    count = pltpu.roll(tot, LANES - 3 * lev, 1)
    lv = pltpu.roll(s, LANES - 4 * lev, 1) / ((members - 1) * cols * ntile)
    bc = s / jnp.maximum(count, 1.0)
    w = jnp.where(lane < lev, lv * bc, 0.0)
    w = w + jnp.where((lane >= lev) & (lane < 2 * lev), pltpu.roll(lv, lev, 1), 0.0)
    lsend[...] = w
    lrecv[my_lev] = w

    def l_copy(d):
        peer = lax.rem(my_lev + d, nlev)
        return pltpu.make_async_remote_copy(
            src_ref=lsend, dst_ref=lrecv.at[my_lev],
            send_sem=l_send.at[d], recv_sem=l_recv.at[my_lev],
            device_id=(me, peer), device_id_type=pl.DeviceIdType.MESH,
        )

    for d in range(1, nlev):
        l_copy(d).start()
    lv_out[...] = lv[0:1, :lev]
    corr_out[...] = jnp.transpose(bc)[:lev, :]
    for d in range(1, nlev):
        src = lax.rem(my_lev + d, nlev)
        pltpu.make_async_copy(lrecv.at[src], lrecv.at[src], l_recv.at[src]).wait()
    all_w = lrecv[0]
    for t in range(1, nlev):
        all_w = all_w + lrecv[t]
    wt = jnp.transpose(all_w)
    num = jnp.sum(wt[:lev], axis=0, keepdims=True)
    den = jnp.sum(wt[lev:2 * lev], axis=0, keepdims=True)
    avg_out[...] = num / den

    for c in halos:
        c.wait_send()
    for d in range(1, ntile):
        t_copy(d).wait_send()
    for d in range(1, nlev):
        l_copy(d).wait_send()


def local(ntile, nlev, ensemble, pair_first, pair_second, pair_bin):
    members, lev, cols = ensemble.shape
    npairs = pair_first.shape[0]
    rows = members * lev
    half = cols // HALO_CHUNKS
    chunks = npairs // PAIR_CHUNK
    total_bins = BIN_DEV * ntile
    f32, bf16 = jnp.float32, jnp.bfloat16
    idx = [x.reshape(npairs // LANES, LANES) for x in (pair_first, pair_second, pair_bin)]
    vmem = pl.BlockSpec(memory_space=pltpu.VMEM)
    hbm = pl.BlockSpec(memory_space=pl.ANY)
    lv, corr, avg = pl.pallas_call(
        functools.partial(kernel, ntile, nlev),
        out_shape=(
            jax.ShapeDtypeStruct((1, lev), f32),
            jax.ShapeDtypeStruct((lev, BIN_DEV), f32),
            jax.ShapeDtypeStruct((1, BIN_DEV), f32),
        ),
        in_specs=[hbm] * 4,
        out_specs=(vmem, vmem, vmem),
        scratch_shapes=[
            pltpu.VMEM((members, lev, cols), bf16),
            pltpu.VMEM((HALO_CHUNKS, members, lev, half), bf16),
            *[pltpu.VMEM((npairs // LANES, LANES), jnp.int32)] * 3,
            pltpu.VMEM((rows + 2 * lev, cols), bf16),
            pltpu.VMEM((HALO_CHUNKS, rows + 2 * lev, half), bf16),
            pltpu.VMEM((lev, cols), f32),
            pltpu.VMEM((chunks, rows, PAIR_CHUNK), f32),
            *[pltpu.VMEM((chunks, lev, PAIR_CHUNK), f32)] * 3,
            pltpu.VMEM((total_bins, LANES), f32),
            pltpu.VMEM((ntile, BIN_DEV, LANES), f32),
            pltpu.VMEM((ntile, BIN_DEV, LANES), f32),
            pltpu.VMEM((BIN_DEV, LANES), f32),
            pltpu.VMEM((nlev, BIN_DEV, LANES), f32),
            pltpu.SemaphoreType.DMA((4,)),
            pltpu.SemaphoreType.DMA((HALO_CHUNKS,)),
            pltpu.SemaphoreType.DMA((HALO_CHUNKS,)),
            pltpu.SemaphoreType.DMA((ntile,)),
            pltpu.SemaphoreType.DMA((ntile,)),
            pltpu.SemaphoreType.DMA((nlev,)),
            pltpu.SemaphoreType.DMA((nlev,)),
        ],
        compiler_params=pltpu.CompilerParams(
            collective_id=0, has_side_effects=True, vmem_limit_bytes=60 * 1024 * 1024
        ),
        name="binned_corr",
    )(ensemble, *idx)
    return lv.reshape(lev), corr, avg.reshape(BIN_DEV)


def solution(mesh):
    in_specs = (P(None, "lev", "tile"), P("tile"), P("tile"), P("tile"))
    out_specs = (P("lev"), P("lev", "tile"), P("tile"))
    body = functools.partial(local, mesh.shape["tile"], mesh.shape["lev"])
    return jax.shard_map(body, mesh=mesh, in_specs=in_specs, out_specs=out_specs, check_vma=False)
```

```python
import functools

import jax
import jax.numpy as jnp
from jax import lax
from jax.experimental import pallas as pl
from jax.experimental.pallas import tpu as pltpu
from jax.sharding import PartitionSpec as P

BIN_DEV = 8
LANES = 128
PAIR_CHUNK = 512
HALO_CHUNKS = 2


def pieces3(x):
    a = x.astype(jnp.bfloat16).astype(jnp.float32)
    r = x - a
    b = r.astype(jnp.bfloat16).astype(jnp.float32)
    return a, b, r - b


def onehot(rows, base, count):
    ids = lax.broadcasted_iota(jnp.int32, (count, LANES), 0) + base
    parts = [jnp.where(ids == r, 1.0, 0.0) for r in rows]
    return jnp.concatenate(parts, axis=1).astype(jnp.bfloat16)


def perturb(raw, out, squares, width):
    members, lev = raw.shape[0], raw.shape[1]
    rows = members * lev
    for c in range(0, width, LANES):
        cs = pl.ds(c, LANES)
        x = raw[:, :, cs].astype(jnp.float32)
        mean = jnp.sum(x, axis=0) / members
        pert = (x - mean[None]).astype(jnp.bfloat16).astype(jnp.float32)
        sq = jnp.sum(pert * pert, axis=0)
        out[pl.ds(0, rows), cs] = pert.reshape(rows, LANES).astype(jnp.bfloat16)
        inv = 1.0 / jnp.sqrt(sq / (members - 1) + 1e-06)
        hi = inv.astype(jnp.bfloat16).astype(jnp.float32)
        out[pl.ds(rows, 2 * lev), cs] = jnp.concatenate([hi, inv - hi], axis=0).astype(jnp.bfloat16)
        if squares is not None:
            squares[:, cs] = sq


def kernel(
    ntile, nlev, ens, first_in, second_in, bin_in, packed,
    raw, halo, first, second, bins, own, nxt, squares, left_buf, cov_buf, ia_buf, ib_buf,
    bin_hot, parts_buf, bacc, sbuf, rbuf, lsend, lrecv,
    load_sem, halo_send, halo_recv, t_send, t_recv, l_send, l_recv,
):
    members, lev, cols = ens.shape
    rows = members * lev
    half = cols // HALO_CHUNKS
    total_bins = BIN_DEV * ntile
    chunks = left_buf.shape[0]
    groups = PAIR_CHUNK // LANES
    me = lax.axis_index("tile")
    my_lev = lax.axis_index("lev")

    barrier = pltpu.get_barrier_semaphore()
    for d in range(1, ntile):
        pl.semaphore_signal(
            barrier, inc=1, device_id=(lax.rem(me + d, ntile), my_lev),
            device_id_type=pl.DeviceIdType.MESH,
        )
    for d in range(1, nlev):
        pl.semaphore_signal(
            barrier, inc=1, device_id=(me, lax.rem(my_lev + d, nlev)),
            device_id_type=pl.DeviceIdType.MESH,
        )
    loads = [
        pltpu.make_async_copy(s, d, load_sem.at[i])
        for i, (s, d) in enumerate(
            ((ens, raw), (first_in, first), (second_in, second), (bin_in, bins))
        )
    ]
    for c in loads:
        c.start()
    loads[0].wait()
    pl.semaphore_wait(barrier, ntile - 1 + nlev - 1)
    prev = lax.rem(me + ntile - 1, ntile)
    halos = [
        pltpu.make_async_remote_copy(
            src_ref=raw.at[:, :, pl.ds(h * half, half)],
            dst_ref=halo.at[h],
            send_sem=halo_send.at[h],
            recv_sem=halo_recv.at[h],
            device_id=(prev, my_lev),
            device_id_type=pl.DeviceIdType.MESH,
        )
        for h in range(HALO_CHUNKS)
    ]
    for c in halos:
        c.start()
    for c in loads[1:]:
        c.wait()

    perturb(raw, own, squares, cols)

    def index_rows(ref, j):
        return [ref[pl.ds(j * groups + i, 1), :] for i in range(groups)]

    def product(a, b):
        return jnp.sum((a * b).reshape(members, lev, PAIR_CHUNK), axis=0)

    def own_step(j, carry):
        x = own[...]
        left = jnp.dot(x, onehot(index_rows(first, j), 0, cols), preferred_element_type=jnp.float32)
        left_buf[j] = left[:rows]
        right = jnp.dot(x, onehot(index_rows(second, j), 0, cols), preferred_element_type=jnp.float32)
        cov_buf[j] = product(left_buf[j], right[:rows])
        ia_buf[j] = left[rows:rows + lev] + left[rows + lev:]
        ib_buf[j] = right[rows:rows + lev] + right[rows + lev:]
        return carry

    lax.fori_loop(0, chunks, own_step, 0)
    def bin_step(j, carry):
        cs = pl.ds(pl.multiple_of(j * PAIR_CHUNK, PAIR_CHUNK), PAIR_CHUNK)
        bin_hot[:, cs] = onehot(index_rows(bins, j), 0, total_bins)
        return carry

    lax.fori_loop(0, chunks, bin_step, 0)
    parts_buf[...] = jnp.zeros_like(parts_buf)

    for h in range(HALO_CHUNKS):
        halos[h].wait_recv()
        perturb(halo.at[h], nxt.at[h], None, half)

        def next_step(j, carry):
            oh = onehot(index_rows(second, j), cols + h * half, half)
            right = jnp.dot(nxt[h], oh, preferred_element_type=jnp.float32)
            cov = cov_buf[j] + product(left_buf[j], right[:rows])
            ib = ib_buf[j] + right[rows:rows + lev] + right[rows + lev:]
            if h < HALO_CHUNKS - 1:
                cov_buf[j] = cov
                ib_buf[j] = ib
            else:
                corr = cov * ia_buf[j] * ib / (members - 1)
                parts = jnp.concatenate(
                    [*pieces3(corr), jnp.ones_like(corr),
                     ], axis=0
                ).astype(jnp.bfloat16)
                parts_buf[pl.ds(0, 4 * lev), pl.ds(pl.multiple_of(j * PAIR_CHUNK, PAIR_CHUNK), PAIR_CHUNK)] = parts
            return carry

        lax.fori_loop(0, chunks, next_step, 0, unroll=4)

    bacc[...] = lax.dot_general(
        bin_hot[...], parts_buf[...], (((1,), (1,)), ((), ())), preferred_element_type=jnp.float32
    )
    sq_parts = jnp.concatenate(
        [jnp.zeros((4 * lev, cols), jnp.float32), *pieces3(squares[...]),
         jnp.zeros((LANES - 7 * lev, cols), jnp.float32)], axis=0
    ).astype(jnp.bfloat16)
    sq_row = lax.dot_general(
        jnp.ones((16, cols), jnp.bfloat16), sq_parts, (((1,), (1,)), ((), ())),
        preferred_element_type=jnp.float32,
    )[:BIN_DEV]
    for t in range(ntile):
        sbuf[t] = bacc[pl.ds(t * BIN_DEV, BIN_DEV), :] + sq_row
    rbuf[me] = sbuf[me]

    def t_copy(d):
        peer = lax.rem(me + d, ntile)
        return pltpu.make_async_remote_copy(
            src_ref=sbuf.at[peer], dst_ref=rbuf.at[me],
            send_sem=t_send.at[d], recv_sem=t_recv.at[me],
            device_id=(peer, my_lev), device_id_type=pl.DeviceIdType.MESH,
        )

    for d in range(1, ntile):
        t_copy(d).start()
    for d in range(1, ntile):
        src = lax.rem(me + d, ntile)
        pltpu.make_async_copy(rbuf.at[src], rbuf.at[src], t_recv.at[src]).wait()
    tot = rbuf[0]
    for t in range(1, ntile):
        tot = tot + rbuf[t]
    lane = lax.broadcasted_iota(jnp.int32, (BIN_DEV, LANES), 1)
    s = tot + pltpu.roll(tot, LANES - lev, 1) + pltpu.roll(tot, LANES - 2 * lev, 1)
    count = pltpu.roll(tot, LANES - 3 * lev, 1)
    lv = pltpu.roll(s, LANES - 4 * lev, 1) / ((members - 1) * cols * ntile)
    bc = s / jnp.maximum(count, 1.0)
    w = jnp.where(lane < lev, lv * bc, 0.0)
    w = w + jnp.where((lane >= lev) & (lane < 2 * lev), pltpu.roll(lv, lev, 1), 0.0)
    lsend[...] = w
    lrecv[my_lev] = w

    def l_copy(d):
        peer = lax.rem(my_lev + d, nlev)
        return pltpu.make_async_remote_copy(
            src_ref=lsend, dst_ref=lrecv.at[my_lev],
            send_sem=l_send.at[d], recv_sem=l_recv.at[my_lev],
            device_id=(me, peer), device_id_type=pl.DeviceIdType.MESH,
        )

    for d in range(1, nlev):
        l_copy(d).start()
    packed[0] = lv
    packed[1] = bc
    for d in range(1, nlev):
        src = lax.rem(my_lev + d, nlev)
        pltpu.make_async_copy(lrecv.at[src], lrecv.at[src], l_recv.at[src]).wait()
    all_w = lrecv[0]
    for t in range(1, nlev):
        all_w = all_w + lrecv[t]
    packed[2] = all_w

    for c in halos:
        c.wait_send()
    for d in range(1, ntile):
        t_copy(d).wait_send()
    for d in range(1, nlev):
        l_copy(d).wait_send()


def unpack(packed, lv_out, corr_out, avg_out):
    lev = corr_out.shape[0]
    lv_out[...] = packed[0, 0:1, :lev]
    corr_out[...] = jnp.transpose(packed[1])[:lev, :]
    wt = jnp.transpose(packed[2])
    num = jnp.sum(wt[:lev], axis=0, keepdims=True)
    den = jnp.sum(wt[lev:2 * lev], axis=0, keepdims=True)
    avg_out[...] = num / den


def local(ntile, nlev, ensemble, pair_first, pair_second, pair_bin):
    members, lev, cols = ensemble.shape
    npairs = pair_first.shape[0]
    rows = members * lev
    half = cols // HALO_CHUNKS
    chunks = npairs // PAIR_CHUNK
    total_bins = BIN_DEV * ntile
    f32, bf16 = jnp.float32, jnp.bfloat16
    idx = [x.reshape(npairs // LANES, LANES) for x in (pair_first, pair_second, pair_bin)]
    vmem = pl.BlockSpec(memory_space=pltpu.VMEM)
    hbm = pl.BlockSpec(memory_space=pl.ANY)
    packed = pl.pallas_call(
        functools.partial(kernel, ntile, nlev),
        out_shape=jax.ShapeDtypeStruct((3, BIN_DEV, LANES), f32),
        in_specs=[hbm] * 4,
        out_specs=vmem,
        scratch_shapes=[
            pltpu.VMEM((members, lev, cols), bf16),
            pltpu.VMEM((HALO_CHUNKS, members, lev, half), bf16),
            *[pltpu.VMEM((npairs // LANES, LANES), jnp.int32)] * 3,
            pltpu.VMEM((rows + 2 * lev, cols), bf16),
            pltpu.VMEM((HALO_CHUNKS, rows + 2 * lev, half), bf16),
            pltpu.VMEM((lev, cols), f32),
            pltpu.VMEM((chunks, rows, PAIR_CHUNK), f32),
            *[pltpu.VMEM((chunks, lev, PAIR_CHUNK), f32)] * 3,
            pltpu.VMEM((total_bins, npairs), bf16),
            pltpu.VMEM((LANES, npairs), bf16),
            pltpu.VMEM((total_bins, LANES), f32),
            pltpu.VMEM((ntile, BIN_DEV, LANES), f32),
            pltpu.VMEM((ntile, BIN_DEV, LANES), f32),
            pltpu.VMEM((BIN_DEV, LANES), f32),
            pltpu.VMEM((nlev, BIN_DEV, LANES), f32),
            pltpu.SemaphoreType.DMA((4,)),
            pltpu.SemaphoreType.DMA((HALO_CHUNKS,)),
            pltpu.SemaphoreType.DMA((HALO_CHUNKS,)),
            pltpu.SemaphoreType.DMA((ntile,)),
            pltpu.SemaphoreType.DMA((ntile,)),
            pltpu.SemaphoreType.DMA((nlev,)),
            pltpu.SemaphoreType.DMA((nlev,)),
        ],
        compiler_params=pltpu.CompilerParams(
            collective_id=0, has_side_effects=True, vmem_limit_bytes=60 * 1024 * 1024
        ),
        name="binned_corr",
    )(ensemble, *idx)
    lv, corr, avg = pl.pallas_call(
        unpack,
        out_shape=(
            jax.ShapeDtypeStruct((1, lev), f32),
            jax.ShapeDtypeStruct((lev, BIN_DEV), f32),
            jax.ShapeDtypeStruct((1, BIN_DEV), f32),
        ),
        in_specs=[vmem],
        out_specs=(vmem, vmem, vmem),
        name="unpack",
    )(packed)
    return lv.reshape(lev), corr, avg.reshape(BIN_DEV)


def solution(mesh):
    in_specs = (P(None, "lev", "tile"), P("tile"), P("tile"), P("tile"))
    out_specs = (P("lev"), P("lev", "tile"), P("tile"))
    body = functools.partial(local, mesh.shape["tile"], mesh.shape["lev"])
    return jax.shard_map(body, mesh=mesh, in_specs=in_specs, out_specs=out_specs, check_vma=False)
```

```python
import functools

import jax
import jax.numpy as jnp
from jax import lax
from jax.experimental import pallas as pl
from jax.experimental.pallas import tpu as pltpu
from jax.sharding import PartitionSpec as P

BIN_DEV = 8
LANES = 128
PAIR_CHUNK = 512
HALO_CHUNKS = 2


def pieces3(x):
    a = x.astype(jnp.bfloat16).astype(jnp.float32)
    r = x - a
    b = r.astype(jnp.bfloat16).astype(jnp.float32)
    return a, b, r - b


def onehot(rows, base, count):
    ids = lax.broadcasted_iota(jnp.int32, (count, LANES), 0) + base
    parts = [jnp.where(ids == r, 1.0, 0.0) for r in rows]
    return jnp.concatenate(parts, axis=1).astype(jnp.bfloat16)


def perturb(raw, out, squares, width):
    members, lev = raw.shape[0], raw.shape[1]
    rows = members * lev
    for c in range(0, width, LANES):
        cs = pl.ds(c, LANES)
        x = raw[:, :, cs].astype(jnp.float32)
        mean = jnp.sum(x, axis=0) / members
        pert = (x - mean[None]).astype(jnp.bfloat16).astype(jnp.float32)
        sq = jnp.sum(pert * pert, axis=0)
        out[pl.ds(0, rows), cs] = pert.reshape(rows, LANES).astype(jnp.bfloat16)
        inv = 1.0 / jnp.sqrt(sq / (members - 1) + 1e-06)
        hi = inv.astype(jnp.bfloat16).astype(jnp.float32)
        out[pl.ds(rows, 2 * lev), cs] = jnp.concatenate([hi, inv - hi], axis=0).astype(jnp.bfloat16)
        if squares is not None:
            squares[:, cs] = sq


def spread_lanes(x, lev):
    lane = lax.broadcasted_iota(jnp.int32, x.shape, 1)
    s = x + pltpu.roll(x, LANES - lev, 1) + pltpu.roll(x, LANES - 2 * lev, 1)
    s = jnp.where(lane < lev, s, 0.0)
    width = lev
    while width < BIN_DEV * lev:
        s = s + pltpu.roll(s, width, 1)
        width *= 2
    return s


def kernel(
    ntile, nlev, ens, first_in, second_in, bin_in, packed,
    raw, halo, first, second, bins, own, nxt, squares, left_buf, cov_buf, ia_buf, ib_buf,
    bin_hot, parts_buf, bacc, sq_buf, sbuf, rbuf,
    load_sem, halo_send, halo_recv, x_send, x_recv, ready,
):
    members, lev, cols = ens.shape
    rows = members * lev
    half = cols // HALO_CHUNKS
    npairs = bin_hot.shape[1]
    total_bins = BIN_DEV * ntile
    chunks = left_buf.shape[0]
    groups = PAIR_CHUNK // LANES
    me = lax.axis_index("tile")
    my_lev = lax.axis_index("lev")

    barrier = pltpu.get_barrier_semaphore()
    for d in range(1, ntile):
        pl.semaphore_signal(
            barrier, inc=1, device_id=(lax.rem(me + d, ntile), my_lev),
            device_id_type=pl.DeviceIdType.MESH,
        )
    for d in range(1, nlev):
        pl.semaphore_signal(
            barrier, inc=1, device_id=(me, lax.rem(my_lev + d, nlev)),
            device_id_type=pl.DeviceIdType.MESH,
        )
    loads = [
        pltpu.make_async_copy(s, d, load_sem.at[i])
        for i, (s, d) in enumerate(
            ((ens, raw), (first_in, first), (second_in, second), (bin_in, bins))
        )
    ]
    for c in loads:
        c.start()
    loads[0].wait()
    pl.semaphore_wait(barrier, ntile - 1 + nlev - 1)
    prev = lax.rem(me + ntile - 1, ntile)
    halos = [
        pltpu.make_async_remote_copy(
            src_ref=raw.at[:, :, pl.ds(h * half, half)],
            dst_ref=halo.at[h],
            send_sem=halo_send.at[h],
            recv_sem=halo_recv.at[h],
            device_id=(prev, my_lev),
            device_id_type=pl.DeviceIdType.MESH,
        )
        for h in range(HALO_CHUNKS)
    ]
    for c in halos:
        c.start()
    for d in range(1, nlev):
        pl.semaphore_signal(
            ready, inc=1, device_id=(me, lax.rem(my_lev + d, nlev)),
            device_id_type=pl.DeviceIdType.MESH,
        )
    for c in loads[1:]:
        c.wait()

    perturb(raw, own, squares, cols)

    def index_rows(ref, j):
        return [ref[pl.ds(j * groups + i, 1), :] for i in range(groups)]

    def product(a, b):
        return jnp.sum((a * b).reshape(members, lev, PAIR_CHUNK), axis=0)

    def own_step(j, carry):
        x = own[...]
        left = jnp.dot(x, onehot(index_rows(first, j), 0, cols), preferred_element_type=jnp.float32)
        left_buf[j] = left[:rows]
        right = jnp.dot(x, onehot(index_rows(second, j), 0, cols), preferred_element_type=jnp.float32)
        cov_buf[j] = product(left_buf[j], right[:rows])
        ia_buf[j] = left[rows:rows + lev] + left[rows + lev:]
        ib_buf[j] = right[rows:rows + lev] + right[rows + lev:]
        return carry

    lax.fori_loop(0, chunks, own_step, 0)
    def bin_step(j, carry):
        cs = pl.ds(pl.multiple_of(j * PAIR_CHUNK, PAIR_CHUNK), PAIR_CHUNK)
        bin_hot[:, cs] = onehot(index_rows(bins, j), 0, total_bins)
        return carry

    lax.fori_loop(0, chunks, bin_step, 0)
    parts_buf[...] = jnp.concatenate(
        [jnp.zeros((BIN_DEV * lev, npairs), jnp.float32), jnp.ones((LANES - BIN_DEV * lev, npairs), jnp.float32)], axis=0
    ).astype(jnp.bfloat16)
    sq_parts = jnp.concatenate(
        [*pieces3(squares[...]), jnp.zeros((LANES - 3 * lev, cols), jnp.float32)], axis=0
    ).astype(jnp.bfloat16)
    sq_row = lax.dot_general(
        jnp.ones((16, cols), jnp.bfloat16), sq_parts, (((1,), (1,)), ((), ())),
        preferred_element_type=jnp.float32,
    )[:BIN_DEV]
    sq_buf[...] = spread_lanes(sq_row, lev)
    pl.semaphore_wait(ready, nlev - 1)

    for h in range(HALO_CHUNKS):
        halos[h].wait_recv()
        perturb(halo.at[h], nxt.at[h], None, half)

        def next_step(j, carry):
            oh = onehot(index_rows(second, j), cols + h * half, half)
            right = jnp.dot(nxt[h], oh, preferred_element_type=jnp.float32)
            cov = cov_buf[j] + product(left_buf[j], right[:rows])
            ib = ib_buf[j] + right[rows:rows + lev] + right[rows + lev:]
            if h < HALO_CHUNKS - 1:
                cov_buf[j] = cov
                ib_buf[j] = ib
            else:
                corr = cov * ia_buf[j] * ib / (members - 1)
                parts = jnp.concatenate(
                    [*pieces3(corr), jnp.zeros_like(corr)], axis=0
                ).astype(jnp.bfloat16)
                parts_buf[pl.ds(0, 4 * lev), pl.ds(pl.multiple_of(j * PAIR_CHUNK, PAIR_CHUNK), PAIR_CHUNK)] = parts
            return carry

        lax.fori_loop(0, chunks, next_step, 0, unroll=4)

    bacc[...] = lax.dot_general(
        bin_hot[...], parts_buf[...], (((1,), (1,)), ((), ())), preferred_element_type=jnp.float32
    )
    half_lanes = BIN_DEV * lev
    wide_lane = lax.broadcasted_iota(jnp.int32, (total_bins, LANES), 1)
    wide = jnp.where(wide_lane < half_lanes, spread_lanes(bacc[...], lev), bacc[...])
    lane = lax.broadcasted_iota(jnp.int32, (BIN_DEV, LANES), 1)
    bin_row = lax.broadcasted_iota(jnp.int32, (BIN_DEV, LANES), 0)
    pick = (lax.rem(lane, half_lanes) // lev == bin_row).astype(jnp.float32)
    for t in range(ntile):
        block = wide[t * BIN_DEV:(t + 1) * BIN_DEV] * pick
        sbuf[t, 0:1, :] = jnp.sum(block, axis=0, keepdims=True)
        sbuf[t, 1:2, :] = sq_buf[0:1, :]
    mine = my_lev * ntile + me
    rbuf[mine] = sbuf[me]

    def x_copy(d):
        dl, dt = d // ntile, d % ntile
        peer_t = lax.rem(me + dt, ntile)
        peer_l = lax.rem(my_lev + dl, nlev)
        return pltpu.make_async_remote_copy(
            src_ref=sbuf.at[peer_t], dst_ref=rbuf.at[mine],
            send_sem=x_send.at[d], recv_sem=x_recv.at[mine],
            device_id=(peer_t, peer_l), device_id_type=pl.DeviceIdType.MESH,
        )

    def x_start(d, carry):
        x_copy(d).start()
        return carry

    def x_wait_send(d, carry):
        x_copy(d).wait_send()
        return carry

    def x_wait(d, carry):
        src = lax.rem(my_lev + d // ntile, nlev) * ntile + lax.rem(me + d % ntile, ntile)
        pltpu.make_async_copy(rbuf.at[src], rbuf.at[src], x_recv.at[src]).wait()
        return carry

    everyone = ntile * nlev
    small = everyone <= 64
    lax.fori_loop(1, everyone, x_start, 0, unroll=small)
    lax.fori_loop(1, everyone, x_wait, 0, unroll=small)
    num = jnp.zeros((1, LANES), jnp.float32)
    den = num
    own_lv = num
    own_bc = num
    for v in range(nlev):
        tot = rbuf[v * ntile]
        for t in range(1, ntile):
            tot = tot + rbuf[v * ntile + t]
        sums, lv = tot[0:1], tot[1:2] / ((members - 1) * cols * ntile)
        bc = sums / jnp.maximum(pltpu.roll(sums, LANES - half_lanes, 1), 1.0)
        num = num + lv * bc
        den = den + lv
        own_lv = jnp.where(my_lev == v, lv, own_lv)
        own_bc = jnp.where(my_lev == v, bc, own_bc)
    for i, row in enumerate((own_lv, own_bc, num, den)):
        packed[i:i + 1, :] = row

    for c in halos:
        c.wait_send()
    lax.fori_loop(1, everyone, x_wait_send, 0, unroll=small)


def unpack(packed, lv_out, corr_out, avg_out):
    lev = corr_out.shape[0]
    lane = lax.broadcasted_iota(jnp.int32, (BIN_DEV, LANES), 1)
    bin_row = lax.broadcasted_iota(jnp.int32, (BIN_DEV, LANES), 0)

    def by_bin(row):
        x = jnp.where(lane // lev == bin_row, row, 0.0)
        return jnp.sum(jnp.transpose(x).reshape(LANES // lev, lev, BIN_DEV), axis=0)

    lv_out[...] = packed[0:1, :lev]
    corr_out[...] = by_bin(packed[1:2, :])
    num = jnp.sum(by_bin(packed[2:3, :]), axis=0, keepdims=True)
    den = jnp.sum(by_bin(packed[3:4, :]), axis=0, keepdims=True)
    avg_out[...] = num / den


def local(ntile, nlev, ensemble, pair_first, pair_second, pair_bin):
    members, lev, cols = ensemble.shape
    npairs = pair_first.shape[0]
    rows = members * lev
    half = cols // HALO_CHUNKS
    chunks = npairs // PAIR_CHUNK
    total_bins = BIN_DEV * ntile
    f32, bf16 = jnp.float32, jnp.bfloat16
    idx = [x.reshape(npairs // LANES, LANES) for x in (pair_first, pair_second, pair_bin)]
    vmem = pl.BlockSpec(memory_space=pltpu.VMEM)
    hbm = pl.BlockSpec(memory_space=pl.ANY)
    packed = pl.pallas_call(
        functools.partial(kernel, ntile, nlev),
        out_shape=jax.ShapeDtypeStruct((8, LANES), f32),
        in_specs=[hbm] * 4,
        out_specs=vmem,
        scratch_shapes=[
            pltpu.VMEM((members, lev, cols), bf16),
            pltpu.VMEM((HALO_CHUNKS, members, lev, half), bf16),
            *[pltpu.VMEM((npairs // LANES, LANES), jnp.int32)] * 3,
            pltpu.VMEM((rows + 2 * lev, cols), bf16),
            pltpu.VMEM((HALO_CHUNKS, rows + 2 * lev, half), bf16),
            pltpu.VMEM((lev, cols), f32),
            pltpu.VMEM((chunks, rows, PAIR_CHUNK), f32),
            *[pltpu.VMEM((chunks, lev, PAIR_CHUNK), f32)] * 3,
            pltpu.VMEM((total_bins, npairs), bf16),
            pltpu.VMEM((LANES, npairs), bf16),
            pltpu.VMEM((total_bins, LANES), f32),
            pltpu.VMEM((BIN_DEV, LANES), f32),
            pltpu.VMEM((ntile, 2, LANES), f32),
            pltpu.VMEM((nlev * ntile, 2, LANES), f32),
            pltpu.SemaphoreType.DMA((4,)),
            pltpu.SemaphoreType.DMA((HALO_CHUNKS,)),
            pltpu.SemaphoreType.DMA((HALO_CHUNKS,)),
            pltpu.SemaphoreType.DMA((nlev * ntile,)),
            pltpu.SemaphoreType.DMA((nlev * ntile,)),
            pltpu.SemaphoreType.REGULAR,
        ],
        compiler_params=pltpu.CompilerParams(
            collective_id=0, has_side_effects=True, vmem_limit_bytes=60 * 1024 * 1024
        ),
        name="binned_corr",
    )(ensemble, *idx)
    lv, corr, avg = pl.pallas_call(
        unpack,
        out_shape=(
            jax.ShapeDtypeStruct((1, lev), f32),
            jax.ShapeDtypeStruct((lev, BIN_DEV), f32),
            jax.ShapeDtypeStruct((1, BIN_DEV), f32),
        ),
        in_specs=[vmem],
        out_specs=(vmem, vmem, vmem),
        name="unpack",
    )(packed)
    return lv.reshape(lev), corr, avg.reshape(BIN_DEV)


def solution(mesh):
    in_specs = (P(None, "lev", "tile"), P("tile"), P("tile"), P("tile"))
    out_specs = (P("lev"), P("lev", "tile"), P("tile"))
    body = functools.partial(local, mesh.shape["tile"], mesh.shape["lev"])
    return jax.shard_map(body, mesh=mesh, in_specs=in_specs, out_specs=out_specs, check_vma=False)
```

```python
import functools

import jax
import jax.numpy as jnp
from jax import lax
from jax.experimental import pallas as pl
from jax.experimental.pallas import tpu as pltpu
from jax.sharding import PartitionSpec as P

BIN_DEV = 8
LANES = 128
PAIR_CHUNK = 512
HALO_CHUNKS = 2


def pieces3(x):
    a = x.astype(jnp.bfloat16).astype(jnp.float32)
    r = x - a
    b = r.astype(jnp.bfloat16).astype(jnp.float32)
    return a, b, r - b


def onehot(rows, base, count):
    ids = lax.broadcasted_iota(jnp.int32, (count, LANES), 0) + base
    parts = [jnp.where(ids == r, 1.0, 0.0) for r in rows]
    return jnp.concatenate(parts, axis=1).astype(jnp.bfloat16)


def perturb(raw, out, squares, width):
    members, lev = raw.shape[0], raw.shape[1]
    rows = members * lev
    for c in range(0, width, LANES):
        cs = pl.ds(c, LANES)
        x = raw[:, :, cs].astype(jnp.float32)
        mean = jnp.sum(x, axis=0) / members
        pert = (x - mean[None]).astype(jnp.bfloat16).astype(jnp.float32)
        sq = jnp.sum(pert * pert, axis=0)
        out[pl.ds(0, rows), cs] = pert.reshape(rows, LANES).astype(jnp.bfloat16)
        inv = 1.0 / jnp.sqrt(sq / (members - 1) + 1e-06)
        hi = inv.astype(jnp.bfloat16).astype(jnp.float32)
        out[pl.ds(rows, 2 * lev), cs] = jnp.concatenate([hi, inv - hi], axis=0).astype(jnp.bfloat16)
        if squares is not None:
            squares[:, cs] = sq


def spread_lanes(x, lev):
    lane = lax.broadcasted_iota(jnp.int32, x.shape, 1)
    s = x + pltpu.roll(x, LANES - lev, 1) + pltpu.roll(x, LANES - 2 * lev, 1)
    s = jnp.where(lane < lev, s, 0.0)
    width = lev
    while width < BIN_DEV * lev:
        s = s + pltpu.roll(s, width, 1)
        width *= 2
    return s


def kernel(
    ntile, nlev, ens, first_in, second_in, bin_in, packed,
    raw, halo, first, second, bins, own, nxt, squares, left_buf, cov_buf, ia_buf, ib_buf,
    bin_hot, parts_buf, bacc, sq_buf, sbuf, rbuf,
    load_sem, halo_send, halo_recv, x_send, x_recv, ready,
):
    members, lev, cols = ens.shape
    rows = members * lev
    half = cols // HALO_CHUNKS
    npairs = bin_hot.shape[1]
    total_bins = BIN_DEV * ntile
    chunks = left_buf.shape[0]
    groups = PAIR_CHUNK // LANES
    me = lax.axis_index("tile")
    my_lev = lax.axis_index("lev")

    barrier = pltpu.get_barrier_semaphore()
    for d in range(1, ntile):
        pl.semaphore_signal(
            barrier, inc=1, device_id=(lax.rem(me + d, ntile), my_lev),
            device_id_type=pl.DeviceIdType.MESH,
        )
    for d in range(1, nlev):
        pl.semaphore_signal(
            barrier, inc=1, device_id=(me, lax.rem(my_lev + d, nlev)),
            device_id_type=pl.DeviceIdType.MESH,
        )
    loads = [
        pltpu.make_async_copy(s, d, load_sem.at[i])
        for i, (s, d) in enumerate(
            ((ens, raw), (first_in, first), (second_in, second), (bin_in, bins))
        )
    ]
    for c in loads:
        c.start()
    loads[0].wait()
    pl.semaphore_wait(barrier, ntile - 1 + nlev - 1)
    prev = lax.rem(me + ntile - 1, ntile)
    halos = [
        pltpu.make_async_remote_copy(
            src_ref=raw.at[:, :, pl.ds(h * half, half)],
            dst_ref=halo.at[h],
            send_sem=halo_send.at[h],
            recv_sem=halo_recv.at[h],
            device_id=(prev, my_lev),
            device_id_type=pl.DeviceIdType.MESH,
        )
        for h in range(HALO_CHUNKS)
    ]
    for c in halos:
        c.start()
    for d in range(1, nlev):
        pl.semaphore_signal(
            ready, inc=1, device_id=(me, lax.rem(my_lev + d, nlev)),
            device_id_type=pl.DeviceIdType.MESH,
        )
    for c in loads[1:]:
        c.wait()

    perturb(raw, own, squares, cols)

    def index_rows(ref, j):
        return [ref[pl.ds(j * groups + i, 1), :] for i in range(groups)]

    def product(a, b):
        return jnp.sum((a * b).reshape(members, lev, PAIR_CHUNK), axis=0)

    def own_step(j, carry):
        x = own[...]
        left = jnp.dot(x, onehot(index_rows(first, j), 0, cols), preferred_element_type=jnp.float32)
        left_buf[j] = left[:rows]
        right = jnp.dot(x, onehot(index_rows(second, j), 0, cols), preferred_element_type=jnp.float32)
        cov_buf[j] = product(left_buf[j], right[:rows])
        ia_buf[j] = left[rows:rows + lev] + left[rows + lev:]
        ib_buf[j] = right[rows:rows + lev] + right[rows + lev:]
        return carry

    lax.fori_loop(0, chunks, own_step, 0)
    def bin_step(j, carry):
        cs = pl.ds(pl.multiple_of(j * PAIR_CHUNK, PAIR_CHUNK), PAIR_CHUNK)
        bin_hot[:, cs] = onehot(index_rows(bins, j), 0, total_bins)
        return carry

    lax.fori_loop(0, chunks, bin_step, 0)
    parts_buf[...] = jnp.concatenate(
        [jnp.zeros((BIN_DEV * lev, npairs), jnp.float32), jnp.ones((LANES - BIN_DEV * lev, npairs), jnp.float32)], axis=0
    ).astype(jnp.bfloat16)
    sq_parts = jnp.concatenate(
        [*pieces3(squares[...]), jnp.zeros((LANES - 3 * lev, cols), jnp.float32)], axis=0
    ).astype(jnp.bfloat16)
    sq_row = lax.dot_general(
        jnp.ones((16, cols), jnp.bfloat16), sq_parts, (((1,), (1,)), ((), ())),
        preferred_element_type=jnp.float32,
    )[:BIN_DEV]
    sq_buf[...] = spread_lanes(sq_row, lev)
    pl.semaphore_wait(ready, nlev - 1)

    for h in range(HALO_CHUNKS):
        halos[h].wait_recv()
        perturb(halo.at[h], nxt.at[h], None, half)

        def next_step(j, carry):
            oh = onehot(index_rows(second, j), cols + h * half, half)
            right = jnp.dot(nxt[h], oh, preferred_element_type=jnp.float32)
            cov = cov_buf[j] + product(left_buf[j], right[:rows])
            ib = ib_buf[j] + right[rows:rows + lev] + right[rows + lev:]
            if h < HALO_CHUNKS - 1:
                cov_buf[j] = cov
                ib_buf[j] = ib
            else:
                corr = cov * ia_buf[j] * ib / (members - 1)
                parts = jnp.concatenate(
                    [*pieces3(corr), jnp.zeros_like(corr)], axis=0
                ).astype(jnp.bfloat16)
                parts_buf[pl.ds(0, 4 * lev), pl.ds(pl.multiple_of(j * PAIR_CHUNK, PAIR_CHUNK), PAIR_CHUNK)] = parts
            return carry

        lax.fori_loop(0, chunks, next_step, 0, unroll=8)

    bacc[...] = lax.dot_general(
        bin_hot[...], parts_buf[...], (((1,), (1,)), ((), ())), preferred_element_type=jnp.float32
    )
    half_lanes = BIN_DEV * lev
    wide_lane = lax.broadcasted_iota(jnp.int32, (total_bins, LANES), 1)
    wide = jnp.where(wide_lane < half_lanes, spread_lanes(bacc[...], lev), bacc[...])
    lane = lax.broadcasted_iota(jnp.int32, (BIN_DEV, LANES), 1)
    bin_row = lax.broadcasted_iota(jnp.int32, (BIN_DEV, LANES), 0)
    pick = (lax.rem(lane, half_lanes) // lev == bin_row).astype(jnp.float32)
    for t in range(ntile):
        block = wide[t * BIN_DEV:(t + 1) * BIN_DEV] * pick
        sbuf[t, 0:1, :] = jnp.sum(block, axis=0, keepdims=True)
        sbuf[t, 1:2, :] = sq_buf[0:1, :]
    mine = my_lev * ntile + me
    rbuf[mine] = sbuf[me]

    def x_copy(d):
        dl, dt = d // ntile, d % ntile
        peer_t = lax.rem(me + dt, ntile)
        peer_l = lax.rem(my_lev + dl, nlev)
        return pltpu.make_async_remote_copy(
            src_ref=sbuf.at[peer_t], dst_ref=rbuf.at[mine],
            send_sem=x_send.at[d], recv_sem=x_recv.at[mine],
            device_id=(peer_t, peer_l), device_id_type=pl.DeviceIdType.MESH,
        )

    def x_start(d, carry):
        x_copy(d).start()
        return carry

    def x_wait_send(d, carry):
        x_copy(d).wait_send()
        return carry

    def x_wait(d, carry):
        src = lax.rem(my_lev + d // ntile, nlev) * ntile + lax.rem(me + d % ntile, ntile)
        pltpu.make_async_copy(rbuf.at[src], rbuf.at[src], x_recv.at[src]).wait()
        return carry

    everyone = ntile * nlev
    small = everyone <= 64
    lax.fori_loop(1, everyone, x_start, 0, unroll=small)
    lax.fori_loop(1, everyone, x_wait, 0, unroll=small)
    num = jnp.zeros((1, LANES), jnp.float32)
    den = num
    own_lv = num
    own_bc = num
    for v in range(nlev):
        tot = rbuf[v * ntile]
        for t in range(1, ntile):
            tot = tot + rbuf[v * ntile + t]
        sums, lv = tot[0:1], tot[1:2] / ((members - 1) * cols * ntile)
        bc = sums / jnp.maximum(pltpu.roll(sums, LANES - half_lanes, 1), 1.0)
        num = num + lv * bc
        den = den + lv
        own_lv = jnp.where(my_lev == v, lv, own_lv)
        own_bc = jnp.where(my_lev == v, bc, own_bc)
    for i, row in enumerate((own_lv, own_bc, num, den)):
        packed[i:i + 1, :] = row

    for c in halos:
        c.wait_send()
    lax.fori_loop(1, everyone, x_wait_send, 0, unroll=small)


def unpack(packed, lv_out, corr_out, avg_out):
    lev = corr_out.shape[0]
    lane = lax.broadcasted_iota(jnp.int32, (BIN_DEV, LANES), 1)
    bin_row = lax.broadcasted_iota(jnp.int32, (BIN_DEV, LANES), 0)

    def by_bin(row):
        x = jnp.where(lane // lev == bin_row, row, 0.0)
        return jnp.sum(jnp.transpose(x).reshape(LANES // lev, lev, BIN_DEV), axis=0)

    lv_out[...] = packed[0:1, :lev]
    corr_out[...] = by_bin(packed[1:2, :])
    num = jnp.sum(by_bin(packed[2:3, :]), axis=0, keepdims=True)
    den = jnp.sum(by_bin(packed[3:4, :]), axis=0, keepdims=True)
    avg_out[...] = num / den


def local(ntile, nlev, ensemble, pair_first, pair_second, pair_bin):
    members, lev, cols = ensemble.shape
    npairs = pair_first.shape[0]
    rows = members * lev
    half = cols // HALO_CHUNKS
    chunks = npairs // PAIR_CHUNK
    total_bins = BIN_DEV * ntile
    f32, bf16 = jnp.float32, jnp.bfloat16
    idx = [x.reshape(npairs // LANES, LANES) for x in (pair_first, pair_second, pair_bin)]
    vmem = pl.BlockSpec(memory_space=pltpu.VMEM)
    hbm = pl.BlockSpec(memory_space=pl.ANY)
    packed = pl.pallas_call(
        functools.partial(kernel, ntile, nlev),
        out_shape=jax.ShapeDtypeStruct((8, LANES), f32),
        in_specs=[hbm] * 4,
        out_specs=vmem,
        scratch_shapes=[
            pltpu.VMEM((members, lev, cols), bf16),
            pltpu.VMEM((HALO_CHUNKS, members, lev, half), bf16),
            *[pltpu.VMEM((npairs // LANES, LANES), jnp.int32)] * 3,
            pltpu.VMEM((rows + 2 * lev, cols), bf16),
            pltpu.VMEM((HALO_CHUNKS, rows + 2 * lev, half), bf16),
            pltpu.VMEM((lev, cols), f32),
            pltpu.VMEM((chunks, rows, PAIR_CHUNK), f32),
            *[pltpu.VMEM((chunks, lev, PAIR_CHUNK), f32)] * 3,
            pltpu.VMEM((total_bins, npairs), bf16),
            pltpu.VMEM((LANES, npairs), bf16),
            pltpu.VMEM((total_bins, LANES), f32),
            pltpu.VMEM((BIN_DEV, LANES), f32),
            pltpu.VMEM((ntile, 2, LANES), f32),
            pltpu.VMEM((nlev * ntile, 2, LANES), f32),
            pltpu.SemaphoreType.DMA((4,)),
            pltpu.SemaphoreType.DMA((HALO_CHUNKS,)),
            pltpu.SemaphoreType.DMA((HALO_CHUNKS,)),
            pltpu.SemaphoreType.DMA((nlev * ntile,)),
            pltpu.SemaphoreType.DMA((nlev * ntile,)),
            pltpu.SemaphoreType.REGULAR,
        ],
        compiler_params=pltpu.CompilerParams(
            collective_id=0, has_side_effects=True, vmem_limit_bytes=60 * 1024 * 1024
        ),
        name="binned_corr",
    )(ensemble, *idx)
    lv, corr, avg = pl.pallas_call(
        unpack,
        out_shape=(
            jax.ShapeDtypeStruct((1, lev), f32),
            jax.ShapeDtypeStruct((lev, BIN_DEV), f32),
            jax.ShapeDtypeStruct((1, BIN_DEV), f32),
        ),
        in_specs=[vmem],
        out_specs=(vmem, vmem, vmem),
        name="unpack",
    )(packed)
    return lv.reshape(lev), corr, avg.reshape(BIN_DEV)


def solution(mesh):
    in_specs = (P(None, "lev", "tile"), P("tile"), P("tile"), P("tile"))
    out_specs = (P("lev"), P("lev", "tile"), P("tile"))
    body = functools.partial(local, mesh.shape["tile"], mesh.shape["lev"])
    return jax.shard_map(body, mesh=mesh, in_specs=in_specs, out_specs=out_specs, check_vma=False)
```
